32 devices in a mesh: zero: 8 (over z, x), tp: 4 (over y, core).
Axes of the slice: x: 2, y: 2, z: 4, core: 2. Of those that a mesh axis runs over, the one named last changes fastest.
Arguments:
- train_gate: float32 [2048, 8192], P('zero', 'tp'), may hold values from -0.1875 to 0.1875
- slow_gate: float32 [2048, 8192], P('zero', 'tp'), may hold values from -0.125 to 0.125
- train_up: float32 [2048, 8192], P('zero', 'tp'), may hold values from -0.1875 to 0.1875
- slow_up: float32 [2048, 8192], P('zero', 'tp'), may hold values from -0.125 to 0.125
- norm_gain: float32 [2048], P('zero'), may hold values from 0.25 to 1.75
Outputs:
- serving_gate: bfloat16 [2048, 8192], P(None, 'tp')
- serving_up: bfloat16 [2048, 8192], P(None, 'tp')
- scale_gate: float32 [8192], P('tp')
- scale_up: float32 [8192], P('tp')
The draws below stay inside these ranges and needn't reach their ends.
All inputs are finite; a program needn't handle non-finite values.
Results may differ from the reference program's by a relative error of at most 0.0004.
Values may be sent and summed in bfloat16 or wider, within the bound.
A program may use at most 128 MiB of HBM per device.

```python
import jax
import jax.numpy as jnp
from jax import lax

D_MODEL = 2048
D_INNER = 8192


def spiked(drawn, key, source, target, shards_of, factor):
    def block_of(axis_at):
        return (jnp.arange(drawn.shape[axis_at]) // (drawn.shape[axis_at] // shards_of)).reshape((-1,) + (1,) * (drawn.ndim - 1 - axis_at))

    near = jax.random.permutation(key, shards_of)[block_of(target)]
    second = (block_of(target) + shards_of // 2) % shards_of
    return jnp.where((block_of(source) == near) | (block_of(source) == second), factor * drawn, drawn)


def block_scale(own_key, dims, split, least, largest):
    gain, own = 1.0, jax.random.fold_in(own_key, 6)
    for dim, parts in split:
        draws = jnp.exp(jax.random.uniform(jax.random.fold_in(own, dim), (parts,), jnp.float32, least / len(split), largest / len(split)))
        gain = gain * jnp.repeat(draws, dims[dim] // parts).reshape([-1 if axis == dim else 1 for axis in range(len(dims))])
    return gain


def gaussian(rng, shape, scale, most, cuts=(), held_as=jnp.bfloat16):
    factor_of = block_scale(rng, shape, cuts, -0.22, 0.18) if cuts else 1.0
    array = jax.random.normal(rng, shape, jnp.float32) * scale * factor_of
    return jnp.minimum(jnp.maximum(array, -most), most).astype(held_as)


def gaussian_with(stream_key, dims, width, bound, pieces, heavy, held_as=jnp.bfloat16):
    array = width * jax.random.normal(stream_key, dims, jnp.float32)
    if pieces:
        array = array * block_scale(stream_key, dims, pieces, -0.22, 0.18)
    return jnp.clip(spiked(array, jax.random.fold_in(stream_key, 3), *heavy), -bound, bound).astype(held_as)


def setup_inputs(seed: int = 0) -> dict:
    arg_keys = jax.random.split(jax.random.key(seed), 6)
    train_gate = gaussian_with(arg_keys[0], (D_MODEL, D_INNER), D_MODEL ** -0.5, 0.1875, ((0, 8), (1, 4)), (0, 1, 8, 2.0), jnp.float32)
    slow_gate = gaussian(arg_keys[1], (D_MODEL, D_INNER), D_MODEL ** -0.5, 0.125, ((0, 8), (1, 4)), jnp.float32)
    train_up = gaussian_with(arg_keys[2], (D_MODEL, D_INNER), D_MODEL ** -0.5, 0.1875, ((0, 8), (1, 4)), (0, 1, 8, 2.0), jnp.float32)
    slow_up = gaussian(arg_keys[3], (D_MODEL, D_INNER), D_MODEL ** -0.5, 0.125, ((0, 8), (1, 4)), jnp.float32)
    norm_gain = jnp.clip(1.0 + 0.15 * jax.random.normal(arg_keys[4], (D_MODEL,), jnp.float32), 0.25, 1.75)
    return {"train_gate": train_gate, "slow_gate": slow_gate, "train_up": train_up, "slow_up": slow_up, "norm_gain": norm_gain}


keep_rate = 0.75

def reference(train_gate, slow_gate, train_up, slow_up, norm_gain):
    whole_gate = keep_rate * slow_gate + (1.0 - keep_rate) * train_gate
    whole_up = keep_rate * slow_up + (1.0 - keep_rate) * train_up
    whole_gained_gate = whole_gate * norm_gain[:, None]
    whole_gained_up = whole_up * norm_gain[:, None]
    scale_gate = jnp.sqrt(lax.optimization_barrier(jnp.sum(whole_gained_gate * whole_gained_gate, axis=0)))
    serving_gate = (whole_gained_gate / scale_gate).astype(jnp.bfloat16)
    scale_up = jnp.sqrt(lax.optimization_barrier(jnp.sum(whole_gained_up * whole_gained_up, axis=0)))
    serving_up = (whole_gained_up / scale_up).astype(jnp.bfloat16)
    return (serving_gate, serving_up, scale_gate, scale_up)
```

```python
import functools

import jax
import jax.numpy as jnp
from jax import lax
from jax.experimental import pallas as pl
from jax.experimental.pallas import tpu as pltpu
from jax.sharding import PartitionSpec as P

keep_rate = 0.75
MESH = pl.DeviceIdType.MESH
SIDE = 2
LANES = 128
GROUP = 8
HEAD = 16
LEAD = 16
SHARES = 16
GATE_RUNS = ((8, 0, False), (16, 0, True))
UP_RUNS = ((3, 0, False), (6, 0, True), (12, 1, False), (16, 2, True))
VMEM_BYTES = 67_043_328


def both(*conditions):
    kept = [c for c in conditions if c is not None]
    return functools.reduce(jnp.logical_and, kept) if kept else None


def when(condition):
    return (lambda f: f()) if condition is None else pl.when(condition)


class Relay:
    def __init__(self, count, rows, head, units, sources, outs, sems):
        self.rows, self.head, self.units, self.sources, self.outs = rows, head, units, sources, outs
        self.left_send, self.left_recv, self.right_send, self.right_recv, self.side_send, self.side_recv, self.half_send, self.half_recv = sems
        me = lax.axis_index("zero")
        self.length = count // SIDE
        self.place, self.side = me // SIDE, me % SIDE
        place, side, length = self.place, self.side, self.length
        self.to_left = jnp.maximum(place - 1, 0) * SIDE + side
        self.to_right = jnp.minimum(place + 1, length - 1) * SIDE + side
        self.to_side = place * SIDE + (SIDE - 1 - side)
        self.has_left, self.has_right = place > 0, place < length - 1
        self.is_even = place % 2 == 0
        self.twin = place + 1 - 2 * (place % 2)
        self.to_twin = self.twin * SIDE + side
        self.half_round = jnp.maximum(jnp.where(self.is_even, place, length - 1 - place), 1)

    def skipped(self, distance, u):
        return self.head if (distance, *self.units[u][:2]) == (0, 0, 0) else 0

    def copy(self, place, side, distance, u, send, recv, to, skip):
        which, first, size = self.units[u][:3]
        start = (place * SIDE + side) * self.rows + first + skip
        at = pl.ds(pl.multiple_of(start, GROUP * 2), size - skip)
        source = self.sources[which] if distance == 0 else self.outs[which]
        return pltpu.make_async_remote_copy(
            src_ref=source.at[at], dst_ref=self.outs[which].at[at], send_sem=send, recv_sem=recv,
            device_id={"zero": to}, device_id_type=MESH,
        )

    def index(self, distance, u):
        return distance * len(self.units) + u

    def left_copy(self, distance, u):
        k = self.index(distance, u)
        return self.copy(self.place + distance, self.side, distance, u, self.left_send.at[k], self.left_recv.at[k], self.to_left, self.skipped(distance, u))

    def left_arrival(self, distance, u):
        k = self.index(distance - 1, u)
        return self.copy(self.place + distance, self.side, 1, u, self.left_send.at[k], self.left_recv.at[k], self.to_right, self.skipped(distance - 1, u))

    def right_copy(self, distance, u):
        k = self.index(distance, u)
        return self.copy(self.place - distance, self.side, distance, u, self.right_send.at[k], self.right_recv.at[k], self.to_right, self.skipped(distance, u))

    def right_arrival(self, distance, u):
        k = self.index(distance - 1, u)
        return self.copy(self.place - distance, self.side, 1, u, self.right_send.at[k], self.right_recv.at[k], self.to_left, self.skipped(distance - 1, u))

    def side_index(self, distance, u):
        return self.index(distance if distance >= 0 else self.length - 1 - distance, u)

    def side_copy(self, distance, u):
        k = self.side_index(distance, u)
        return self.copy(self.place + distance, self.side, distance, u, self.side_send.at[k], self.side_recv.at[k], self.to_side, self.skipped(distance, u))

    def side_arrival(self, distance, u):
        k = self.side_index(distance, u)
        return self.copy(self.place + distance, SIDE - 1 - self.side, 1, u, self.side_send.at[k], self.side_recv.at[k], self.to_side, self.skipped(distance, u))

    def half_copy(self, u):
        return self.copy(self.place, SIDE - 1 - self.side, 1, u, self.half_send.at[u], self.half_recv.at[u], self.to_twin, 0)

    def half_arrival(self, u):
        return self.copy(self.twin, SIDE - 1 - self.side, 1, u, self.half_send.at[u], self.half_recv.at[u], self.to_twin, 0)

    def is_half(self, u):
        return self.units[u][4]

    def in_line(self, distance):
        return self.place + distance <= self.length - 1 if distance > 0 else self.place + distance >= 0

    def by_side(self, distance, u):
        ok = self.in_line(distance)
        if self.is_half(u) and distance == 1:
            ok = jnp.logical_and(ok, jnp.logical_not(self.is_even))
        if self.is_half(u) and distance == -1:
            ok = jnp.logical_and(ok, self.is_even)
        return ok

    def send_own(self, u):
        condition = self.units[u][3]

        @when(both(condition, self.has_left))
        def _():
            self.left_copy(0, u).start()

        @when(both(condition, self.has_right))
        def _():
            self.right_copy(0, u).start()

        @when(condition)
        def _():
            self.side_copy(0, u).start()

    def forward(self):
        everything = range(len(self.units))
        for k in range(1, self.length):
            for u in everything:
                condition = self.units[u][3]

                @when(both(condition, self.in_line(k)))
                def _():
                    self.left_arrival(k, u).wait_recv()

                    @pl.when(self.has_left)
                    def _():
                        self.left_copy(k, u).start()

                @when(both(condition, self.by_side(k, u)))
                def _():
                    self.side_copy(k, u).start()

                @when(both(condition, self.in_line(-k)))
                def _():
                    self.right_arrival(k, u).wait_recv()

                    @pl.when(self.has_right)
                    def _():
                        self.right_copy(k, u).start()

                @when(both(condition, self.by_side(-k, u)))
                def _():
                    self.side_copy(-k, u).start()

            for u in everything:
                if self.is_half(u):
                    @when(both(self.units[u][3], self.half_round == k))
                    def _():
                        self.side_arrival(0, u).wait_recv()
                        self.half_copy(u).start()

    def finish(self):
        everything = range(len(self.units))
        for u in everything:
            if not self.is_half(u):
                @when(self.units[u][3])
                def _():
                    self.side_arrival(0, u).wait_recv()

        for k in range(1, self.length):
            for u in everything:
                for distance in (k, -k):
                    @when(both(self.units[u][3], self.by_side(distance, u)))
                    def _():
                        self.side_arrival(distance, u).wait_recv()
                        self.side_copy(distance, u).wait_send()

        for u in everything:
            if self.is_half(u):
                @when(self.units[u][3])
                def _():
                    self.half_arrival(u).wait_recv()
                    self.half_copy(u).wait_send()

        for u in everything:
            condition = self.units[u][3]

            @when(condition)
            def _():
                self.side_copy(0, u).wait_send()

            for k in range(self.length):
                @when(both(condition, self.has_left, self.place + k <= self.length - 1))
                def _():
                    self.left_copy(k, u).wait_send()

                @when(both(condition, self.has_right, self.place - k >= 0))
                def _():
                    self.right_copy(k, u).wait_send()


def is_late():
    return lax.axis_index("tp") % 2 == 1


def plan(rows):
    def cut(share):
        return share * rows // SHARES // 16 * 16

    units = []
    for which, runs in enumerate((GATE_RUNS, UP_RUNS)):
        last = 0
        for end, when, halved in runs:
            if cut(end) > cut(last):
                units.append((which, cut(last), cut(end) - cut(last), when, halved))
            last = end
    return units


def first_units(rows):
    late = is_late()
    return [(which, first, size, late if when else None, halved) for which, first, size, when, halved in plan(rows) if when < 2]


def last_units(rows):
    early = jnp.logical_not(is_late())
    return [(which, first, size, early if when < 2 else None, halved) for which, first, size, when, halved in plan(rows) if when]


def first_kernel(
    count, pieces, head,
    train_gate, slow_gate, train_up, slow_up, gain_ref,
    gate_ref, up_ref, scale_gate_ref, scale_up_ref,
    train, slow, gains, sums, heads,
    head_send, head_recv, load_sem, sum_send, sum_recv, *sems,
):
    rows, columns = train_gate.shape
    piece_rows = rows // pieces
    me = lax.axis_index("zero")
    outs = (gate_ref, up_ref)
    scales = (scale_gate_ref, scale_up_ref)
    relay = Relay(count, rows, head, first_units(rows), outs, outs, sems)

    barrier = pltpu.get_barrier_semaphore()
    for step in range(1, count):
        pl.semaphore_signal(barrier, 1, device_id={"zero": lax.rem(me + step, count)}, device_id_type=MESH)

    loads = []
    for which, (t, s) in enumerate(((train_gate, slow_gate), (train_up, slow_up))):
        for p in range(pieces):
            at = pl.ds(p * piece_rows, piece_rows)
            k = (which * pieces + p) * 2
            loads.append((
                pltpu.make_async_copy(t.at[at], train.at[which, at], load_sem.at[k]),
                pltpu.make_async_copy(s.at[at], slow.at[which, at], load_sem.at[k + 1]),
            ))
    for pair in loads:
        for load in pair:
            load.start()

    gains[...] = jnp.broadcast_to(gain_ref[...], (LANES, rows)).T

    def sum_copy(which, step, source, to):
        k = which * (count - 1) + step - 1
        return pltpu.make_async_remote_copy(
            src_ref=sums.at[which, source], dst_ref=sums.at[which, source],
            send_sem=sum_send.at[k], recv_sem=sum_recv.at[k],
            device_id={"zero": to}, device_id_type=MESH,
        )

    for which in range(2):
        def add(i, total):
            at = pl.ds(pl.multiple_of(i * GROUP, GROUP), GROUP)
            gain = jnp.concatenate([gains[at, :]] * (columns // LANES), axis=1)
            gained = (keep_rate * slow[which, at, :] + (1.0 - keep_rate) * train[which, at, :]) * gain
            slow[which, at, :] = gained
            return total + gained * gained

        total = jnp.zeros((GROUP, columns), jnp.float32)
        for p in range(pieces):
            for load in loads[which * pieces + p]:
                load.wait()
            total = lax.fori_loop(p * piece_rows // GROUP, (p + 1) * piece_rows // GROUP, add, total)
        sums[which, me] = jnp.sum(total, axis=0, keepdims=True)
        if which == 0:
            pl.semaphore_wait(barrier, count - 1)
        for step in range(1, count):
            sum_copy(which, step, me, lax.rem(me + step, count)).start()

    def head_copy(slot, to):
        return pltpu.make_async_remote_copy(
            src_ref=slow.at[0, pl.ds(0, head)], dst_ref=heads.at[slot],
            send_sem=head_send.at[slot], recv_sem=head_recv.at[slot],
            device_id={"zero": to}, device_id_type=MESH,
        )

    @pl.when(relay.has_left)
    def _():
        head_copy(0, relay.to_left).start()

    @pl.when(relay.has_right)
    def _():
        head_copy(1, relay.to_right).start()

    head_copy(2, relay.to_side).start()

    for which in range(2):
        for step in range(1, count):
            source = lax.rem(me + count - step, count)
            sum_copy(which, step, source, source).wait_recv()
        total = sums[which, 0]
        for k in range(1, count):
            total = total + sums[which, k]
        scale = jnp.sqrt(total)
        scales[which][...] = scale
        inverse = 1.0 / scale

        def store(first, size):
            start = pl.multiple_of(me * rows + first, GROUP * 2)
            block = slow[which, pl.ds(first, size), :]
            outs[which][pl.ds(start, size), :] = (block * inverse).astype(jnp.bfloat16)

        mine = [(u, unit[1], unit[2]) for u, unit in enumerate(relay.units) if unit[0] == which]
        stored = 0
        for u, first, size in mine:
            ready = min(first + size + LEAD, rows)
            if ready > stored:
                store(stored, ready - stored)
            relay.send_own(u)
            stored = ready
        if stored < rows:
            store(stored, rows - stored)

        if which == 0:
            def use_head(slot, owner, sender):
                head_copy(slot, sender).wait_recv()
                start = pl.multiple_of(owner * rows, GROUP * 2)
                outs[0][pl.ds(start, head), :] = (heads[slot] * inverse).astype(jnp.bfloat16)

            @pl.when(relay.has_right)
            def _():
                use_head(0, relay.to_right, relay.to_right)

            @pl.when(relay.has_left)
            def _():
                use_head(1, relay.to_left, relay.to_left)

            use_head(2, relay.to_side, relay.to_side)

    relay.forward()
    relay.finish()

    for which in range(2):
        for step in range(1, count):
            sum_copy(which, step, me, lax.rem(me + step, count)).wait_send()

    @pl.when(relay.has_left)
    def _():
        head_copy(0, relay.to_left).wait_send()

    @pl.when(relay.has_right)
    def _():
        head_copy(1, relay.to_right).wait_send()

    head_copy(2, relay.to_side).wait_send()


def last_kernel(count, own_ref, token_ref, up_ref, *sems):
    rows = own_ref.shape[0] // count
    relay = Relay(count, rows, 0, last_units(rows), (None, own_ref), (None, up_ref), sems)
    barrier = pltpu.get_barrier_semaphore()

    def greet(to):
        pl.semaphore_signal(barrier, 1, device_id={"zero": to}, device_id_type=MESH)

    @pl.when(relay.has_left)
    def _():
        greet(relay.to_left)

    @pl.when(relay.has_right)
    def _():
        greet(relay.to_right)

    greet(relay.to_side)
    pl.semaphore_wait(barrier, 1 + relay.has_left.astype(jnp.int32) + relay.has_right.astype(jnp.int32))
    for u in range(len(relay.units)):
        relay.send_own(u)
    relay.forward()
    relay.finish()


def phases(rows):
    found = []
    for phase in range(3):
        units = [unit for unit in plan(rows) if unit[0] == 1 and unit[3] == phase]
        if units:
            found.append((phase, units[0][1], sum(unit[2] for unit in units)))
    return found


def run_copies(copies):
    for condition, copy in copies:
        when(condition)(copy.start)
    for condition, copy in copies:
        when(condition)(copy.wait)


def first_store_kernel(count, parts, gate, up, scale_gate, scale_up, gate_out, up_out, scale_gate_out, scale_up_out, token, sem):
    token[...] = jnp.zeros_like(token)
    me, late = lax.axis_index("zero"), is_late()
    rows = up.shape[0] // count
    copies = []

    def add(condition, held, out):
        copies.append((condition, pltpu.make_async_copy(held, out, sem.at[len(copies)])))

    whole = gate.shape[0] // parts
    for k in range(parts):
        at = pl.ds(k * whole, whole)
        add(None, gate.at[at], gate_out.at[at])
    for owner in range(count):
        for phase, first, size in phases(rows):
            at = pl.ds(owner * rows + first, size)
            condition = (None, jnp.logical_or(late, me == owner), me == owner)[phase]
            add(condition, up.at[at], up_out.at[at])
    add(None, scale_gate.at[0], scale_gate_out)
    add(None, scale_up.at[0], scale_up_out)
    run_copies(copies)


def last_store_kernel(count, up, up_before, up_out, sem):
    me, early = lax.axis_index("zero"), jnp.logical_not(is_late())
    rows = up.shape[0] // count
    copies = []
    for owner in range(count):
        for phase, first, size in phases(rows):
            if phase:
                at = pl.ds(owner * rows + first, size)
                condition = jnp.logical_and(early, me != owner) if phase == 1 else me != owner
                copies.append((condition, pltpu.make_async_copy(up.at[at], up_out.at[at], sem.at[len(copies)])))
    run_copies(copies)


def solution(mesh):
    count = mesh.shape["zero"]

    def body(train_gate, slow_gate, train_up, slow_up, norm_gain):
        rows, columns = train_gate.shape
        pieces = max(1, min(2, rows // 64))
        whens = [unit[3] for unit in plan(rows)]
        length = count // SIDE
        full = (rows * count, columns)
        block = pltpu.VMEM(full, jnp.bfloat16)
        scale = pltpu.VMEM((1, columns), jnp.float32)
        token = pltpu.VMEM((GROUP, LANES), jnp.float32)
        wide = jax.ShapeDtypeStruct(full, jnp.bfloat16)
        vmem, held = pl.BlockSpec(memory_space=pltpu.VMEM), pl.BlockSpec(memory_space=pltpu.HBM)
        dma = lambda n: pltpu.SemaphoreType.DMA((n,))

        def relay_sems(n):
            line, across = length * n, (2 * length - 1) * n
            return [dma(line), dma(line), dma(line), dma(line), dma(across), dma(across), dma(n), dma(n)]

        gate, up, scale_gate, scale_up = pl.pallas_call(
            functools.partial(first_kernel, count, pieces, HEAD),
            out_shape=(block, block, scale, scale),
            in_specs=[held] * 4 + [vmem],
            out_specs=(vmem,) * 4,
            scratch_shapes=[
                pltpu.VMEM((2, rows, columns), jnp.float32),
                pltpu.VMEM((2, rows, columns), jnp.float32),
                pltpu.VMEM((rows, LANES), jnp.float32),
                pltpu.VMEM((2, count, 1, columns), jnp.float32),
                pltpu.VMEM((3, HEAD, columns), jnp.float32),
                dma(3), dma(3), dma(4 * pieces), dma(2 * count - 2), dma(2 * count - 2),
                *relay_sems(sum(when < 2 for when in whens)),
            ],
            compiler_params=pltpu.CompilerParams(
                collective_id=0, has_side_effects=True,
                vmem_limit_bytes=VMEM_BYTES - 3 * full[0] * full[1] * 2 - (1 << 20),
            ),
        )(train_gate, slow_gate, train_up, slow_up, norm_gain[None, :])
        parts = 4
        flat = jax.ShapeDtypeStruct((columns,), jnp.float32)
        gate_out, up_out, scale_gate, scale_up, token = pl.pallas_call(
            functools.partial(first_store_kernel, count, parts),
            out_shape=(wide, wide, flat, flat, token),
            in_specs=[vmem] * 4,
            out_specs=(held,) * 4 + (vmem,),
            scratch_shapes=[dma(parts + 3 * count + 2)],
            compiler_params=pltpu.CompilerParams(vmem_limit_bytes=1 << 20),
        )(gate, up, scale_gate, scale_up)
        rest = pl.pallas_call(
            functools.partial(last_kernel, count),
            out_shape=block,
            in_specs=[vmem, vmem],
            out_specs=vmem,
            scratch_shapes=relay_sems(sum(when > 0 for when in whens)),
            compiler_params=pltpu.CompilerParams(collective_id=1, has_side_effects=True, vmem_limit_bytes=1 << 20),
        )(up, token)
        up_out = pl.pallas_call(
            functools.partial(last_store_kernel, count),
            out_shape=wide,
            in_specs=[vmem, held],
            out_specs=held,
            scratch_shapes=[dma(2 * count)],
            input_output_aliases={1: 0},
            compiler_params=pltpu.CompilerParams(vmem_limit_bytes=1 << 20),
        )(rest, up_out)
        return gate_out, up_out, scale_gate, scale_up

    in_specs = (P("zero", "tp"), P("zero", "tp"), P("zero", "tp"), P("zero", "tp"), P("zero"))
    out_specs = (P(None, "tp"), P(None, "tp"), P("tp"), P("tp"))
    return jax.shard_map(body, mesh=mesh, in_specs=in_specs, out_specs=out_specs, check_vma=False)
```

```python
import functools

import jax
import jax.numpy as jnp
from jax import lax
from jax.experimental import pallas as pl
from jax.experimental.pallas import tpu as pltpu
from jax.sharding import PartitionSpec as P

keep_rate = 0.75
MESH = pl.DeviceIdType.MESH
SIDE = 2
LANES = 128
GROUP = 8
HEAD = 16
LEAD = 16
SHARES = 16
GATE_RUNS = ((10, 0, False), (16, 0, True))
UP_RUNS = ((5, 0, True), (12, 1, False), (16, 2, True))
VMEM_BYTES = 67_043_328


def both(*conditions):
    kept = [c for c in conditions if c is not None]
    return functools.reduce(jnp.logical_and, kept) if kept else None


def when(condition):
    return (lambda f: f()) if condition is None else pl.when(condition)


class Relay:
    def __init__(self, count, rows, head, units, sources, outs, sems):
        self.rows, self.head, self.units, self.sources, self.outs = rows, head, units, sources, outs
        self.left_send, self.left_recv, self.right_send, self.right_recv, self.side_send, self.side_recv, self.half_send, self.half_recv = sems
        me = lax.axis_index("zero")
        self.length = count // SIDE
        self.place, self.side = me // SIDE, me % SIDE
        place, side, length = self.place, self.side, self.length
        self.to_left = jnp.maximum(place - 1, 0) * SIDE + side
        self.to_right = jnp.minimum(place + 1, length - 1) * SIDE + side
        self.to_side = place * SIDE + (SIDE - 1 - side)
        self.has_left, self.has_right = place > 0, place < length - 1
        self.is_even = place % 2 == 0
        self.twin = place + 1 - 2 * (place % 2)
        self.to_twin = self.twin * SIDE + side
        self.is_inner = both(place > 0, place < length - 1)
        self.twin_is_inner = both(self.twin > 0, self.twin < length - 1)
        self.half_round = jnp.maximum(jnp.where(self.is_even, place, length - 1 - place), 1)

    def skipped(self, distance, u):
        return self.head if (distance, *self.units[u][:2]) == (0, 0, 0) else 0

    def copy(self, place, side, distance, u, send, recv, to, skip):
        which, first, size = self.units[u][:3]
        start = (place * SIDE + side) * self.rows + first + skip
        at = pl.ds(pl.multiple_of(start, GROUP * 2), size - skip)
        source = self.sources[which] if distance == 0 else self.outs[which]
        return pltpu.make_async_remote_copy(
            src_ref=source.at[at], dst_ref=self.outs[which].at[at], send_sem=send, recv_sem=recv,
            device_id={"zero": to}, device_id_type=MESH,
        )

    def index(self, distance, u):
        return distance * len(self.units) + u

    def left_copy(self, distance, u):
        k = self.index(distance, u)
        return self.copy(self.place + distance, self.side, distance, u, self.left_send.at[k], self.left_recv.at[k], self.to_left, self.skipped(distance, u))

    def left_arrival(self, distance, u):
        k = self.index(distance - 1, u)
        return self.copy(self.place + distance, self.side, 1, u, self.left_send.at[k], self.left_recv.at[k], self.to_right, self.skipped(distance - 1, u))

    def right_copy(self, distance, u):
        k = self.index(distance, u)
        return self.copy(self.place - distance, self.side, distance, u, self.right_send.at[k], self.right_recv.at[k], self.to_right, self.skipped(distance, u))

    def right_arrival(self, distance, u):
        k = self.index(distance - 1, u)
        return self.copy(self.place - distance, self.side, 1, u, self.right_send.at[k], self.right_recv.at[k], self.to_left, self.skipped(distance - 1, u))

    def side_index(self, distance, u):
        return self.index(distance if distance >= 0 else self.length - 1 - distance, u)

    def side_copy(self, distance, u):
        k = self.side_index(distance, u)
        return self.copy(self.place + distance, self.side, distance, u, self.side_send.at[k], self.side_recv.at[k], self.to_side, self.skipped(distance, u))

    def side_arrival(self, distance, u):
        k = self.side_index(distance, u)
        return self.copy(self.place + distance, SIDE - 1 - self.side, 1, u, self.side_send.at[k], self.side_recv.at[k], self.to_side, self.skipped(distance, u))

    def half_copy(self, u):
        return self.copy(self.place, SIDE - 1 - self.side, 1, u, self.half_send.at[u], self.half_recv.at[u], self.to_twin, 0)

    def half_arrival(self, u):
        return self.copy(self.twin, SIDE - 1 - self.side, 1, u, self.half_send.at[u], self.half_recv.at[u], self.to_twin, 0)

    def is_half(self, u):
        return self.units[u][4]

    def in_line(self, distance):
        return self.place + distance <= self.length - 1 if distance > 0 else self.place + distance >= 0

    def gets_half(self, u):
        return None if self.is_half(u) else self.is_inner

    def sends_half(self, u):
        return None if self.is_half(u) else self.twin_is_inner

    def by_side(self, distance, u):
        ok = self.in_line(distance)
        if distance in (1, -1):
            is_twin = self.is_even if distance == 1 else jnp.logical_not(self.is_even)
            ok = jnp.logical_and(ok, jnp.logical_not(both(is_twin, self.gets_half(u))))
        return ok

    def send_own(self, u):
        condition = self.units[u][3]

        @when(both(condition, self.has_left))
        def _():
            self.left_copy(0, u).start()

        @when(both(condition, self.has_right))
        def _():
            self.right_copy(0, u).start()

        @when(condition)
        def _():
            self.side_copy(0, u).start()

    def forward(self):
        everything = range(len(self.units))
        for k in range(1, self.length):
            for u in everything:
                condition = self.units[u][3]

                @when(both(condition, self.in_line(k)))
                def _():
                    self.left_arrival(k, u).wait_recv()

                    @pl.when(self.has_left)
                    def _():
                        self.left_copy(k, u).start()

                @when(both(condition, self.by_side(k, u)))
                def _():
                    self.side_copy(k, u).start()

                @when(both(condition, self.in_line(-k)))
                def _():
                    self.right_arrival(k, u).wait_recv()

                    @pl.when(self.has_right)
                    def _():
                        self.right_copy(k, u).start()

                @when(both(condition, self.by_side(-k, u)))
                def _():
                    self.side_copy(-k, u).start()

            for u in everything:
                @when(both(self.units[u][3], self.half_round == k, self.sends_half(u)))
                def _():
                    self.side_arrival(0, u).wait_recv()
                    self.half_copy(u).start()

    def finish(self):
        everything = range(len(self.units))

        def end_half(u):
            @when(both(self.units[u][3], self.gets_half(u)))
            def _():
                self.half_arrival(u).wait_recv()

            @when(both(self.units[u][3], self.sends_half(u)))
            def _():
                self.half_copy(u).wait_send()

        for k in range(self.length):
            if k == self.length - 1:
                for u in everything:
                    if not self.is_half(u):
                        end_half(u)

            for u in everything:
                condition = self.units[u][3]

                @when(both(condition, self.has_left, self.place + k <= self.length - 1))
                def _():
                    self.left_copy(k, u).wait_send()

                @when(both(condition, self.has_right, self.place - k >= 0))
                def _():
                    self.right_copy(k, u).wait_send()

                if k == 0:
                    @when(condition)
                    def _():
                        self.side_copy(0, u).wait_send()

                    if not self.is_half(u):
                        @when(both(condition, jnp.logical_not(self.twin_is_inner)))
                        def _():
                            self.side_arrival(0, u).wait_recv()
                else:
                    for distance in (k, -k):
                        @when(both(condition, self.by_side(distance, u)))
                        def _():
                            self.side_arrival(distance, u).wait_recv()
                            self.side_copy(distance, u).wait_send()

        for u in everything:
            if self.is_half(u):
                end_half(u)


def is_late():
    return lax.axis_index("tp") % 2 == 1


def plan(rows):
    def cut(share):
        return share * rows // SHARES // 16 * 16

    units = []
    for which, runs in enumerate((GATE_RUNS, UP_RUNS)):
        last = 0
        for end, when, halved in runs:
            if cut(end) > cut(last):
                units.append((which, cut(last), cut(end) - cut(last), when, halved))
            last = end
    return units


def first_units(rows):
    late = is_late()
    return [(which, first, size, late if when else None, halved) for which, first, size, when, halved in plan(rows) if when < 2]


def last_units(rows):
    early = jnp.logical_not(is_late())
    return [(which, first, size, early if when < 2 else None, halved) for which, first, size, when, halved in plan(rows) if when]


def first_kernel(
    count, pieces, head,
    train_gate, slow_gate, train_up, slow_up, gain_ref,
    gate_ref, up_ref, scale_gate_ref, scale_up_ref,
    train, slow, gains, sums, heads,
    head_send, head_recv, load_sem, sum_send, sum_recv, *sems,
):
    rows, columns = train_gate.shape
    piece_rows = rows // pieces
    me = lax.axis_index("zero")
    outs = (gate_ref, up_ref)
    scales = (scale_gate_ref, scale_up_ref)
    relay = Relay(count, rows, head, first_units(rows), outs, outs, sems)

    barrier = pltpu.get_barrier_semaphore()
    for step in range(1, count):
        pl.semaphore_signal(barrier, 1, device_id={"zero": lax.rem(me + step, count)}, device_id_type=MESH)

    loads = []
    for which, (t, s) in enumerate(((train_gate, slow_gate), (train_up, slow_up))):
        for p in range(pieces):
            at = pl.ds(p * piece_rows, piece_rows)
            k = (which * pieces + p) * 2
            loads.append((
                pltpu.make_async_copy(t.at[at], train.at[which, at], load_sem.at[k]),
                pltpu.make_async_copy(s.at[at], slow.at[which, at], load_sem.at[k + 1]),
            ))
    for pair in loads:
        for load in pair:
            load.start()

    gains[...] = jnp.broadcast_to(gain_ref[...], (LANES, rows)).T

    def sum_copy(which, step, source, to):
        k = which * (count - 1) + step - 1
        return pltpu.make_async_remote_copy(
            src_ref=sums.at[which, source], dst_ref=sums.at[which, source],
            send_sem=sum_send.at[k], recv_sem=sum_recv.at[k],
            device_id={"zero": to}, device_id_type=MESH,
        )

    def head_copy(slot, to):
        return pltpu.make_async_remote_copy(
            src_ref=slow.at[0, pl.ds(0, head)], dst_ref=heads.at[slot],
            send_sem=head_send.at[slot], recv_sem=head_recv.at[slot],
            device_id={"zero": to}, device_id_type=MESH,
        )

    def send_heads():
        @pl.when(relay.has_left)
        def _():
            head_copy(0, relay.to_left).start()

        @pl.when(relay.has_right)
        def _():
            head_copy(1, relay.to_right).start()

        head_copy(2, relay.to_side).start()

    for which in range(2):
        def add(i, total):
            at = pl.ds(pl.multiple_of(i * GROUP, GROUP), GROUP)
            gain = jnp.concatenate([gains[at, :]] * (columns // LANES), axis=1)
            gained = (keep_rate * slow[which, at, :] + (1.0 - keep_rate) * train[which, at, :]) * gain
            slow[which, at, :] = gained
            return total + gained * gained

        total = jnp.zeros((GROUP, columns), jnp.float32)
        for p in range(pieces):
            for load in loads[which * pieces + p]:
                load.wait()
            total = lax.fori_loop(p * piece_rows // GROUP, (p + 1) * piece_rows // GROUP, add, total, unroll=2)
        sums[which, me] = jnp.sum(total, axis=0, keepdims=True)
        if which == 0:
            pl.semaphore_wait(barrier, count - 1)
        for step in range(1, count):
            sum_copy(which, step, me, lax.rem(me + step, count)).start()
        if which == 0:
            send_heads()

    for which in range(2):
        for step in range(1, count):
            source = lax.rem(me + count - step, count)
            sum_copy(which, step, source, source).wait_recv()
        total = sums[which, 0]
        for k in range(1, count):
            total = total + sums[which, k]
        scale = jnp.sqrt(total)
        scales[which][...] = scale
        inverse = 1.0 / scale

        def store(first, size):
            start = pl.multiple_of(me * rows + first, GROUP * 2)
            block = slow[which, pl.ds(first, size), :]
            outs[which][pl.ds(start, size), :] = (block * inverse).astype(jnp.bfloat16)

        mine = [(u, unit[1], unit[2]) for u, unit in enumerate(relay.units) if unit[0] == which]
        stored = 0
        for u, first, size in mine:
            ready = min(first + size + LEAD, rows)
            if ready > stored:
                store(stored, ready - stored)
            relay.send_own(u)
            stored = ready
        if stored < rows:
            store(stored, rows - stored)

        if which == 0:
            def use_head(slot, owner, sender):
                head_copy(slot, sender).wait_recv()
                start = pl.multiple_of(owner * rows, GROUP * 2)
                outs[0][pl.ds(start, head), :] = (heads[slot] * inverse).astype(jnp.bfloat16)

            @pl.when(relay.has_right)
            def _():
                use_head(0, relay.to_right, relay.to_right)

            @pl.when(relay.has_left)
            def _():
                use_head(1, relay.to_left, relay.to_left)

            use_head(2, relay.to_side, relay.to_side)

    for which in range(2):
        for step in range(1, count):
            sum_copy(which, step, me, lax.rem(me + step, count)).wait_send()

    @pl.when(relay.has_left)
    def _():
        head_copy(0, relay.to_left).wait_send()

    @pl.when(relay.has_right)
    def _():
        head_copy(1, relay.to_right).wait_send()

    head_copy(2, relay.to_side).wait_send()
    relay.forward()
    relay.finish()


def last_kernel(count, own_ref, token_ref, up_ref, *sems):
    rows = own_ref.shape[0] // count
    relay = Relay(count, rows, 0, last_units(rows), (None, own_ref), (None, up_ref), sems)
    barrier = pltpu.get_barrier_semaphore()

    def greet(to):
        pl.semaphore_signal(barrier, 1, device_id={"zero": to}, device_id_type=MESH)

    @pl.when(relay.has_left)
    def _():
        greet(relay.to_left)

    @pl.when(relay.has_right)
    def _():
        greet(relay.to_right)

    greet(relay.to_side)
    pl.semaphore_wait(barrier, 1 + relay.has_left.astype(jnp.int32) + relay.has_right.astype(jnp.int32))
    for u in range(len(relay.units)):
        relay.send_own(u)
    relay.forward()
    relay.finish()


def phases(rows):
    found = []
    for phase in range(3):
        units = [unit for unit in plan(rows) if unit[0] == 1 and unit[3] == phase]
        if units:
            found.append((phase, units[0][1], sum(unit[2] for unit in units)))
    return found


def run_copies(copies):
    for condition, copy in copies:
        when(condition)(copy.start)
    for condition, copy in copies:
        when(condition)(copy.wait)


def first_store_kernel(count, parts, gate, up, scale_gate, scale_up, gate_out, up_out, scale_gate_out, scale_up_out, token, sem):
    token[...] = jnp.zeros_like(token)
    me, late = lax.axis_index("zero"), is_late()
    rows = up.shape[0] // count
    copies = []

    def add(condition, held, out):
        copies.append((condition, pltpu.make_async_copy(held, out, sem.at[len(copies)])))

    whole = gate.shape[0] // parts
    for k in range(parts):
        at = pl.ds(k * whole, whole)
        add(None, gate.at[at], gate_out.at[at])
    for owner in range(count):
        for phase, first, size in phases(rows):
            at = pl.ds(owner * rows + first, size)
            condition = (None, jnp.logical_or(late, me == owner), me == owner)[phase]
            add(condition, up.at[at], up_out.at[at])
    add(None, scale_gate.at[0], scale_gate_out)
    add(None, scale_up.at[0], scale_up_out)
    run_copies(copies)


def last_store_kernel(count, up, up_before, up_out, sem):
    me, early = lax.axis_index("zero"), jnp.logical_not(is_late())
    rows = up.shape[0] // count
    copies = []
    for owner in range(count):
        for phase, first, size in phases(rows):
            if phase:
                at = pl.ds(owner * rows + first, size)
                condition = jnp.logical_and(early, me != owner) if phase == 1 else me != owner
                copies.append((condition, pltpu.make_async_copy(up.at[at], up_out.at[at], sem.at[len(copies)])))
    run_copies(copies)


def solution(mesh):
    count = mesh.shape["zero"]

    def body(train_gate, slow_gate, train_up, slow_up, norm_gain):
        rows, columns = train_gate.shape
        pieces = max(1, min(4, rows // 64))
        whens = [unit[3] for unit in plan(rows)]
        length = count // SIDE
        full = (rows * count, columns)
        block = pltpu.VMEM(full, jnp.bfloat16)
        scale = pltpu.VMEM((1, columns), jnp.float32)
        token = pltpu.VMEM((GROUP, LANES), jnp.float32)
        wide = jax.ShapeDtypeStruct(full, jnp.bfloat16)
        vmem, held = pl.BlockSpec(memory_space=pltpu.VMEM), pl.BlockSpec(memory_space=pltpu.HBM)
        dma = lambda n: pltpu.SemaphoreType.DMA((n,))

        def relay_sems(n):
            line, across = length * n, (2 * length - 1) * n
            return [dma(line), dma(line), dma(line), dma(line), dma(across), dma(across), dma(n), dma(n)]

        gate, up, scale_gate, scale_up = pl.pallas_call(
            functools.partial(first_kernel, count, pieces, HEAD),
            out_shape=(block, block, scale, scale),
            in_specs=[held] * 4 + [vmem],
            out_specs=(vmem,) * 4,
            scratch_shapes=[
                pltpu.VMEM((2, rows, columns), jnp.float32),
                pltpu.VMEM((2, rows, columns), jnp.float32),
                pltpu.VMEM((rows, LANES), jnp.float32),
                pltpu.VMEM((2, count, 1, columns), jnp.float32),
                pltpu.VMEM((3, HEAD, columns), jnp.float32),
                dma(3), dma(3), dma(4 * pieces), dma(2 * count - 2), dma(2 * count - 2),
                *relay_sems(sum(when < 2 for when in whens)),
            ],
            compiler_params=pltpu.CompilerParams(
                collective_id=0, has_side_effects=True,
                vmem_limit_bytes=VMEM_BYTES - 3 * full[0] * full[1] * 2 - (1 << 20),
            ),
        )(train_gate, slow_gate, train_up, slow_up, norm_gain[None, :])
        parts = 4
        flat = jax.ShapeDtypeStruct((columns,), jnp.float32)
        gate_out, up_out, scale_gate, scale_up, token = pl.pallas_call(
            functools.partial(first_store_kernel, count, parts),
            out_shape=(wide, wide, flat, flat, token),
            in_specs=[vmem] * 4,
            out_specs=(held,) * 4 + (vmem,),
            scratch_shapes=[dma(parts + 3 * count + 2)],
            compiler_params=pltpu.CompilerParams(vmem_limit_bytes=1 << 20),
        )(gate, up, scale_gate, scale_up)
        rest = pl.pallas_call(
            functools.partial(last_kernel, count),
            out_shape=block,
            in_specs=[vmem, vmem],
            out_specs=vmem,
            scratch_shapes=relay_sems(sum(when > 0 for when in whens)),
            compiler_params=pltpu.CompilerParams(collective_id=1, has_side_effects=True, vmem_limit_bytes=1 << 20),
        )(up, token)
        up_out = pl.pallas_call(
            functools.partial(last_store_kernel, count),
            out_shape=wide,
            in_specs=[vmem, held],
            out_specs=held,
            scratch_shapes=[dma(2 * count)],
            input_output_aliases={1: 0},
            compiler_params=pltpu.CompilerParams(vmem_limit_bytes=1 << 20),
        )(rest, up_out)
        return gate_out, up_out, scale_gate, scale_up

    in_specs = (P("zero", "tp"), P("zero", "tp"), P("zero", "tp"), P("zero", "tp"), P("zero"))
    out_specs = (P(None, "tp"), P(None, "tp"), P("tp"), P("tp"))
    return jax.shard_map(body, mesh=mesh, in_specs=in_specs, out_specs=out_specs, check_vma=False)
```

```python
import functools

import jax
import jax.numpy as jnp
from jax import lax
from jax.experimental import pallas as pl
from jax.experimental.pallas import tpu as pltpu
from jax.sharding import PartitionSpec as P

keep_rate = 0.75
MESH = pl.DeviceIdType.MESH
SIDE = 2
LANES = 128
GROUP = 8
HEAD = 16
LEAD = 16
SHARES = 16
GATE_RUNS = ((5, 0, False), (16, 0, True))
UP_RUNS = ((5, 0, False), (12, 1, False), (16, 2, True))
VMEM_BYTES = 67_043_328


def both(*conditions):
    kept = [c for c in conditions if c is not None]
    return functools.reduce(jnp.logical_and, kept) if kept else None


def when(condition):
    return (lambda f: f()) if condition is None else pl.when(condition)


class Relay:
    def __init__(self, count, rows, head, units, sources, outs, sems):
        self.rows, self.head, self.units, self.sources, self.outs = rows, head, units, sources, outs
        self.left_send, self.left_recv, self.right_send, self.right_recv, self.side_send, self.side_recv, self.half_send, self.half_recv = sems
        me = lax.axis_index("zero")
        self.length = count // SIDE
        self.place, self.side = me // SIDE, me % SIDE
        place, side, length = self.place, self.side, self.length
        self.to_left = jnp.maximum(place - 1, 0) * SIDE + side
        self.to_right = jnp.minimum(place + 1, length - 1) * SIDE + side
        self.to_side = place * SIDE + (SIDE - 1 - side)
        self.has_left, self.has_right = place > 0, place < length - 1
        self.is_even = place % 2 == 0
        self.twin = place + 1 - 2 * (place % 2)
        self.to_twin = self.twin * SIDE + side
        self.is_inner = both(place > 0, place < length - 1)
        self.twin_is_inner = both(self.twin > 0, self.twin < length - 1)
        self.half_round = jnp.maximum(jnp.where(self.is_even, place, length - 1 - place), 1)

    def skipped(self, distance, u):
        return self.head if (distance, *self.units[u][:2]) == (0, 0, 0) else 0

    def copy(self, place, side, distance, u, send, recv, to, skip):
        which, first, size = self.units[u][:3]
        start = (place * SIDE + side) * self.rows + first + skip
        at = pl.ds(pl.multiple_of(start, GROUP * 2), size - skip)
        source = self.sources[which] if distance == 0 else self.outs[which]
        return pltpu.make_async_remote_copy(
            src_ref=source.at[at], dst_ref=self.outs[which].at[at], send_sem=send, recv_sem=recv,
            device_id={"zero": to}, device_id_type=MESH,
        )

    def index(self, distance, u):
        return distance * len(self.units) + u

    def left_copy(self, distance, u):
        k = self.index(distance, u)
        return self.copy(self.place + distance, self.side, distance, u, self.left_send.at[k], self.left_recv.at[k], self.to_left, self.skipped(distance, u))

    def left_arrival(self, distance, u):
        k = self.index(distance - 1, u)
        return self.copy(self.place + distance, self.side, 1, u, self.left_send.at[k], self.left_recv.at[k], self.to_right, self.skipped(distance - 1, u))

    def right_copy(self, distance, u):
        k = self.index(distance, u)
        return self.copy(self.place - distance, self.side, distance, u, self.right_send.at[k], self.right_recv.at[k], self.to_right, self.skipped(distance, u))

    def right_arrival(self, distance, u):
        k = self.index(distance - 1, u)
        return self.copy(self.place - distance, self.side, 1, u, self.right_send.at[k], self.right_recv.at[k], self.to_left, self.skipped(distance - 1, u))

    def side_index(self, distance, u):
        return self.index(distance if distance >= 0 else self.length - 1 - distance, u)

    def side_copy(self, distance, u):
        k = self.side_index(distance, u)
        return self.copy(self.place + distance, self.side, distance, u, self.side_send.at[k], self.side_recv.at[k], self.to_side, self.skipped(distance, u))

    def side_arrival(self, distance, u):
        k = self.side_index(distance, u)
        return self.copy(self.place + distance, SIDE - 1 - self.side, 1, u, self.side_send.at[k], self.side_recv.at[k], self.to_side, self.skipped(distance, u))

    def half_copy(self, u):
        return self.copy(self.place, SIDE - 1 - self.side, 1, u, self.half_send.at[u], self.half_recv.at[u], self.to_twin, 0)

    def half_arrival(self, u):
        return self.copy(self.twin, SIDE - 1 - self.side, 1, u, self.half_send.at[u], self.half_recv.at[u], self.to_twin, 0)

    def is_half(self, u):
        return self.units[u][4]

    def in_line(self, distance):
        return self.place + distance <= self.length - 1 if distance > 0 else self.place + distance >= 0

    def gets_half(self, u):
        return None if self.is_half(u) else self.is_inner

    def sends_half(self, u):
        return None if self.is_half(u) else self.twin_is_inner

    def by_side(self, distance, u):
        ok = self.in_line(distance)
        if distance in (1, -1):
            is_twin = self.is_even if distance == 1 else jnp.logical_not(self.is_even)
            ok = jnp.logical_and(ok, jnp.logical_not(both(is_twin, self.gets_half(u))))
        return ok

    def send_own(self, u):
        condition = self.units[u][3]

        @when(both(condition, self.has_left))
        def _():
            self.left_copy(0, u).start()

        @when(both(condition, self.has_right))
        def _():
            self.right_copy(0, u).start()

        @when(condition)
        def _():
            self.side_copy(0, u).start()

    def forward(self):
        everything = range(len(self.units))
        for k in range(1, self.length):
            for u in everything:
                condition = self.units[u][3]

                @when(both(condition, self.in_line(k)))
                def _():
                    self.left_arrival(k, u).wait_recv()

                    @pl.when(self.has_left)
                    def _():
                        self.left_copy(k, u).start()

                @when(both(condition, self.by_side(k, u)))
                def _():
                    self.side_copy(k, u).start()

                @when(both(condition, self.in_line(-k)))
                def _():
                    self.right_arrival(k, u).wait_recv()

                    @pl.when(self.has_right)
                    def _():
                        self.right_copy(k, u).start()

                @when(both(condition, self.by_side(-k, u)))
                def _():
                    self.side_copy(-k, u).start()

            for u in everything:
                @when(both(self.units[u][3], self.half_round == k, self.sends_half(u)))
                def _():
                    self.side_arrival(0, u).wait_recv()
                    self.half_copy(u).start()

    def finish(self):
        everything = range(len(self.units))

        def end_half(u):
            @when(both(self.units[u][3], self.gets_half(u)))
            def _():
                self.half_arrival(u).wait_recv()

            @when(both(self.units[u][3], self.sends_half(u)))
            def _():
                self.half_copy(u).wait_send()

        for k in range(self.length):
            if k == self.length - 1:
                for u in everything:
                    if not self.is_half(u):
                        end_half(u)

            for u in everything:
                condition = self.units[u][3]

                @when(both(condition, self.has_left, self.place + k <= self.length - 1))
                def _():
                    self.left_copy(k, u).wait_send()

                @when(both(condition, self.has_right, self.place - k >= 0))
                def _():
                    self.right_copy(k, u).wait_send()

                if k == 0:
                    @when(condition)
                    def _():
                        self.side_copy(0, u).wait_send()

                    if not self.is_half(u):
                        @when(both(condition, jnp.logical_not(self.twin_is_inner)))
                        def _():
                            self.side_arrival(0, u).wait_recv()
                else:
                    for distance in (k, -k):
                        @when(both(condition, self.by_side(distance, u)))
                        def _():
                            self.side_arrival(distance, u).wait_recv()
                            self.side_copy(distance, u).wait_send()

        for u in everything:
            if self.is_half(u):
                end_half(u)


def is_late():
    return lax.axis_index("tp") % 2 == 1


def plan(rows):
    def cut(share):
        return share * rows // SHARES // 16 * 16

    units = []
    for which, runs in enumerate((GATE_RUNS, UP_RUNS)):
        last = 0
        for end, when, halved in runs:
            if cut(end) > cut(last):
                units.append((which, cut(last), cut(end) - cut(last), when, halved))
            last = end
    return units


def first_units(rows):
    late = is_late()
    return [(which, first, size, late if when else None, halved) for which, first, size, when, halved in plan(rows) if when < 2]


def last_units(rows):
    early = jnp.logical_not(is_late())
    return [(which, first, size, early if when < 2 else None, halved) for which, first, size, when, halved in plan(rows) if when]


def first_kernel(
    count, pieces, head,
    train_gate, slow_gate, train_up, slow_up, gain_ref,
    gate_ref, up_ref, scale_gate_ref, scale_up_ref,
    train, slow, gains, sums, heads,
    head_send, head_recv, load_sem, sum_send, sum_recv, *sems,
):
    rows, columns = train_gate.shape
    piece_rows = rows // pieces
    me = lax.axis_index("zero")
    outs = (gate_ref, up_ref)
    scales = (scale_gate_ref, scale_up_ref)
    relay = Relay(count, rows, head, first_units(rows), outs, outs, sems)

    barrier = pltpu.get_barrier_semaphore()
    for step in range(1, count):
        pl.semaphore_signal(barrier, 1, device_id={"zero": lax.rem(me + step, count)}, device_id_type=MESH)

    loads = []
    for which, (t, s) in enumerate(((train_gate, slow_gate), (train_up, slow_up))):
        for p in range(pieces):
            at = pl.ds(p * piece_rows, piece_rows)
            k = (which * pieces + p) * 2
            loads.append((
                pltpu.make_async_copy(t.at[at], train.at[which, at], load_sem.at[k]),
                pltpu.make_async_copy(s.at[at], slow.at[which, at], load_sem.at[k + 1]),
            ))
    for pair in loads:
        for load in pair:
            load.start()

    gains[...] = jnp.broadcast_to(gain_ref[...], (LANES, rows)).T

    def sum_copy(which, step, source, to):
        k = which * (count - 1) + step - 1
        return pltpu.make_async_remote_copy(
            src_ref=sums.at[which, source], dst_ref=sums.at[which, source],
            send_sem=sum_send.at[k], recv_sem=sum_recv.at[k],
            device_id={"zero": to}, device_id_type=MESH,
        )

    def head_copy(slot, to):
        return pltpu.make_async_remote_copy(
            src_ref=slow.at[0, pl.ds(0, head)], dst_ref=heads.at[slot],
            send_sem=head_send.at[slot], recv_sem=head_recv.at[slot],
            device_id={"zero": to}, device_id_type=MESH,
        )

    def send_heads():
        @pl.when(relay.has_left)
        def _():
            head_copy(0, relay.to_left).start()

        @pl.when(relay.has_right)
        def _():
            head_copy(1, relay.to_right).start()

        head_copy(2, relay.to_side).start()

    for which in range(2):
        def add(i, total):
            at = pl.ds(pl.multiple_of(i * GROUP, GROUP), GROUP)
            gain = jnp.concatenate([gains[at, :]] * (columns // LANES), axis=1)
            gained = (keep_rate * slow[which, at, :] + (1.0 - keep_rate) * train[which, at, :]) * gain
            slow[which, at, :] = gained
            return total + gained * gained

        total = jnp.zeros((GROUP, columns), jnp.float32)
        for p in range(pieces):
            for load in loads[which * pieces + p]:
                load.wait()
            total = lax.fori_loop(p * piece_rows // GROUP, (p + 1) * piece_rows // GROUP, add, total, unroll=2)
        sums[which, me] = jnp.sum(total, axis=0, keepdims=True)
        if which == 0:
            pl.semaphore_wait(barrier, count - 1)
        for step in range(1, count):
            sum_copy(which, step, me, lax.rem(me + step, count)).start()
        if which == 0:
            send_heads()

    for which in range(2):
        for step in range(1, count):
            source = lax.rem(me + count - step, count)
            sum_copy(which, step, source, source).wait_recv()
        total = sums[which, 0]
        for k in range(1, count):
            total = total + sums[which, k]
        scale = jnp.sqrt(total)
        scales[which][...] = scale
        inverse = 1.0 / scale

        def store(first, size):
            start = pl.multiple_of(me * rows + first, GROUP * 2)
            block = slow[which, pl.ds(first, size), :]
            outs[which][pl.ds(start, size), :] = (block * inverse).astype(jnp.bfloat16)

        mine = [(u, unit[1], unit[2]) for u, unit in enumerate(relay.units) if unit[0] == which]
        stored = 0
        for u, first, size in mine:
            ready = min(first + size + LEAD, rows)
            if ready > stored:
                store(stored, ready - stored)
            relay.send_own(u)
            stored = ready
        if stored < rows:
            store(stored, rows - stored)

        if which == 0:
            def use_head(slot, owner, sender):
                head_copy(slot, sender).wait_recv()
                start = pl.multiple_of(owner * rows, GROUP * 2)
                outs[0][pl.ds(start, head), :] = (heads[slot] * inverse).astype(jnp.bfloat16)

            @pl.when(relay.has_right)
            def _():
                use_head(0, relay.to_right, relay.to_right)

            @pl.when(relay.has_left)
            def _():
                use_head(1, relay.to_left, relay.to_left)

            use_head(2, relay.to_side, relay.to_side)

    for which in range(2):
        for step in range(1, count):
            sum_copy(which, step, me, lax.rem(me + step, count)).wait_send()

    @pl.when(relay.has_left)
    def _():
        head_copy(0, relay.to_left).wait_send()

    @pl.when(relay.has_right)
    def _():
        head_copy(1, relay.to_right).wait_send()

    head_copy(2, relay.to_side).wait_send()
    relay.forward()
    relay.finish()


def last_kernel(count, own_ref, token_ref, up_ref, *sems):
    rows = own_ref.shape[0] // count
    relay = Relay(count, rows, 0, last_units(rows), (None, own_ref), (None, up_ref), sems)
    barrier = pltpu.get_barrier_semaphore()

    def greet(to):
        pl.semaphore_signal(barrier, 1, device_id={"zero": to}, device_id_type=MESH)

    @pl.when(relay.has_left)
    def _():
        greet(relay.to_left)

    @pl.when(relay.has_right)
    def _():
        greet(relay.to_right)

    greet(relay.to_side)
    pl.semaphore_wait(barrier, 1 + relay.has_left.astype(jnp.int32) + relay.has_right.astype(jnp.int32))
    for u in range(len(relay.units)):
        relay.send_own(u)
    relay.forward()
    relay.finish()


def phases(rows):
    found = []
    for phase in range(3):
        units = [unit for unit in plan(rows) if unit[0] == 1 and unit[3] == phase]
        if units:
            found.append((phase, units[0][1], sum(unit[2] for unit in units)))
    return found


def run_copies(copies):
    for condition, copy in copies:
        when(condition)(copy.start)
    for condition, copy in copies:
        when(condition)(copy.wait)


def first_store_kernel(count, parts, gate, up, scale_gate, scale_up, gate_out, up_out, scale_gate_out, scale_up_out, token, sem):
    token[...] = jnp.zeros_like(token)
    me, late = lax.axis_index("zero"), is_late()
    rows = up.shape[0] // count
    copies = []

    def add(condition, held, out):
        copies.append((condition, pltpu.make_async_copy(held, out, sem.at[len(copies)])))

    whole = gate.shape[0] // parts
    for k in range(parts):
        at = pl.ds(k * whole, whole)
        add(None, gate.at[at], gate_out.at[at])
    for owner in range(count):
        for phase, first, size in phases(rows):
            at = pl.ds(owner * rows + first, size)
            condition = (None, jnp.logical_or(late, me == owner), me == owner)[phase]
            add(condition, up.at[at], up_out.at[at])
    add(None, scale_gate.at[0], scale_gate_out)
    add(None, scale_up.at[0], scale_up_out)
    run_copies(copies)


def last_store_kernel(count, up, up_before, up_out, sem):
    me, early = lax.axis_index("zero"), jnp.logical_not(is_late())
    rows = up.shape[0] // count
    copies = []
    for owner in range(count):
        for phase, first, size in phases(rows):
            if phase:
                at = pl.ds(owner * rows + first, size)
                condition = jnp.logical_and(early, me != owner) if phase == 1 else me != owner
                copies.append((condition, pltpu.make_async_copy(up.at[at], up_out.at[at], sem.at[len(copies)])))
    run_copies(copies)


def solution(mesh):
    count = mesh.shape["zero"]

    def body(train_gate, slow_gate, train_up, slow_up, norm_gain):
        rows, columns = train_gate.shape
        pieces = max(1, min(4, rows // 64))
        whens = [unit[3] for unit in plan(rows)]
        length = count // SIDE
        full = (rows * count, columns)
        block = pltpu.VMEM(full, jnp.bfloat16)
        scale = pltpu.VMEM((1, columns), jnp.float32)
        token = pltpu.VMEM((GROUP, LANES), jnp.float32)
        wide = jax.ShapeDtypeStruct(full, jnp.bfloat16)
        vmem, held = pl.BlockSpec(memory_space=pltpu.VMEM), pl.BlockSpec(memory_space=pltpu.HBM)
        dma = lambda n: pltpu.SemaphoreType.DMA((n,))

        def relay_sems(n):
            line, across = length * n, (2 * length - 1) * n
            return [dma(line), dma(line), dma(line), dma(line), dma(across), dma(across), dma(n), dma(n)]

        gate, up, scale_gate, scale_up = pl.pallas_call(
            functools.partial(first_kernel, count, pieces, HEAD),
            out_shape=(block, block, scale, scale),
            in_specs=[held] * 4 + [vmem],
            out_specs=(vmem,) * 4,
            scratch_shapes=[
                pltpu.VMEM((2, rows, columns), jnp.float32),
                pltpu.VMEM((2, rows, columns), jnp.float32),
                pltpu.VMEM((rows, LANES), jnp.float32),
                pltpu.VMEM((2, count, 1, columns), jnp.float32),
                pltpu.VMEM((3, HEAD, columns), jnp.float32),
                dma(3), dma(3), dma(4 * pieces), dma(2 * count - 2), dma(2 * count - 2),
                *relay_sems(sum(when < 2 for when in whens)),
            ],
            compiler_params=pltpu.CompilerParams(
                collective_id=0, has_side_effects=True,
                vmem_limit_bytes=VMEM_BYTES - 3 * full[0] * full[1] * 2 - (1 << 20),
            ),
        )(train_gate, slow_gate, train_up, slow_up, norm_gain[None, :])
        parts = 4
        flat = jax.ShapeDtypeStruct((columns,), jnp.float32)
        gate_out, up_out, scale_gate, scale_up, token = pl.pallas_call(
            functools.partial(first_store_kernel, count, parts),
            out_shape=(wide, wide, flat, flat, token),
            in_specs=[vmem] * 4,
            out_specs=(held,) * 4 + (vmem,),
            scratch_shapes=[dma(parts + 3 * count + 2)],
            compiler_params=pltpu.CompilerParams(vmem_limit_bytes=1 << 20),
        )(gate, up, scale_gate, scale_up)
        rest = pl.pallas_call(
            functools.partial(last_kernel, count),
            out_shape=block,
            in_specs=[vmem, vmem],
            out_specs=vmem,
            scratch_shapes=relay_sems(sum(when > 0 for when in whens)),
            compiler_params=pltpu.CompilerParams(collective_id=1, has_side_effects=True, vmem_limit_bytes=1 << 20),
        )(up, token)
        up_out = pl.pallas_call(
            functools.partial(last_store_kernel, count),
            out_shape=wide,
            in_specs=[vmem, held],
            out_specs=held,
            scratch_shapes=[dma(2 * count)],
            input_output_aliases={1: 0},
            compiler_params=pltpu.CompilerParams(vmem_limit_bytes=1 << 20),
        )(rest, up_out)
        return gate_out, up_out, scale_gate, scale_up

    in_specs = (P("zero", "tp"), P("zero", "tp"), P("zero", "tp"), P("zero", "tp"), P("zero"))
    out_specs = (P(None, "tp"), P(None, "tp"), P("tp"), P("tp"))
    return jax.shard_map(body, mesh=mesh, in_specs=in_specs, out_specs=out_specs, check_vma=False)
```
